256 devices in a mesh: dp: 256 (over z, y, x, core).
Axes of the slice: x: 4, y: 4, z: 8, core: 2. Of those that a mesh axis runs over, the one named last changes fastest.
Arguments:
- grads: float32 [256, 1310720], P('dp'), may hold values from -24 to 24
- master: float32 [1310720], P('dp')
- moment1: float32 [1310720], P('dp'), may hold values from -4 to 4
- moment2: float32 [1310720], P('dp'), may hold values from 0.1 to 2
- tensor_rows: int32 [8], replicated, may hold values from 1 to 128, 256 in all
- step_count: int32 [1], replicated, may hold values from 1 to 19
Outputs:
- new_weights: bfloat16 [1310720], replicated
- new_master: float32 [1310720], P('dp')
- new_moment1: float32 [1310720], P('dp')
- new_moment2: float32 [1310720], P('dp')
The draws below stay inside these ranges and needn't reach their ends.
All inputs are finite; a program needn't handle non-finite values.
Results may differ from the reference program's by a relative error of at most 0.001.
Values may be sent and summed in bfloat16 or wider, within the bound.
A program may use at most 64 MiB of HBM per device.

```python
import math
import jax
import jax.numpy as jnp
import numpy as np
from jax import lax

D = 5120
NSEG = 8
ROWS = 256
P_SIZE = 1310720
N_DP = 256


def draw_master(key, part):
    base_key, row_key, col_key = jax.random.split(jax.random.fold_in(key, 17), 3)
    base = jax.random.normal(base_key, (ROWS, D), jnp.float32)
    position = jnp.arange(ROWS, dtype=jnp.float32) / jnp.float32(ROWS)
    row_scale = jnp.exp(jax.random.uniform(row_key, (ROWS, 1), jnp.float32, 0.0, math.log(10.0)))
    row_scale = row_scale * jnp.power(3.0, position)[:, None]
    col_scale = jnp.exp(jax.random.uniform(col_key, (1, D), jnp.float32, 0.0, math.log(4.0)))
    return (0.1 * base * row_scale * col_scale).reshape(P_SIZE).astype(jnp.float32)


def strengthened(entries, rng, source, target, shards_of, factor):
    def block_of(dim):
        return (jnp.arange(entries.shape[dim]) // (entries.shape[dim] // shards_of)).reshape((-1,) + (1,) * (entries.ndim - 1 - dim))

    first = jax.random.permutation(rng, shards_of)[block_of(target)]
    far = (block_of(target) + shards_of // 2) % shards_of
    return jnp.where((block_of(source) == first) | (block_of(source) == far), factor * entries, entries)


def shard_levels(own_key, extent, pieces, least, largest):
    def one(dim, parts):
        heights = jax.random.uniform(jax.random.fold_in(jax.random.fold_in(own_key, 6), dim), (parts,), jnp.float32, least / len(pieces), largest / len(pieces))
        return jnp.repeat(jnp.exp(heights), extent[dim] // parts).reshape((-1,) + (1,) * (len(extent) - dim - 1))

    factor_of = one(*pieces[0])
    for cut in pieces[1:]:
        factor_of = factor_of * one(*cut)
    return factor_of


def split_up(number_of, total, bound, lean):
    weights = [(1 << 20) // math.isqrt(rank ** lean) + 1 for rank in range(2, number_of + 1)]
    surplus, given = total - bound - (number_of - 1), [1] * (number_of - 1)
    while surplus > 0:
        candidates = [i for i in range(number_of - 1) if given[i] < bound]
        pool, remaining = sum([weights[i] for i in candidates]), surplus
        for i in candidates:
            addition = min(bound - given[i], max(1, remaining * weights[i] // pool), surplus)
            given[i] = given[i] + addition
            surplus = surplus - addition
    return np.array([bound] + given)


def uneven_parts(rng, count, total, most, skew):
    if count == 2:
        one = jax.random.randint(rng, (), max(1, total - most), min(most, total - 1) + 1)
        return jnp.stack([one, total - one])
    sizes = jnp.asarray(split_up(count, total, most, skew), jnp.int32)
    pairs = (count - 1) // 2
    giver, taker = sizes[1:1 + 2 * pairs:2], sizes[2:2 + 2 * pairs:2]
    margin = jnp.minimum(giver - 1, most - taker)
    passed = jax.random.randint(jax.random.fold_in(rng, 1), (pairs,), 0, 1 << 20) % (margin + 1)
    sizes = sizes.at[1:1 + 2 * pairs:2].set(giver - passed).at[2:2 + 2 * pairs:2].set(taker + passed)
    return sizes[jax.random.permutation(jax.random.fold_in(rng, 2), count)]


def noise(own_key, extent, spread, reach, cuts=(), held_as=jnp.bfloat16):
    loudness = shard_levels(own_key, extent, cuts, -0.22, 0.18) if cuts else 1.0
    entries = jax.random.normal(own_key, extent, jnp.float32) * spread * loudness
    return jnp.minimum(jnp.maximum(entries, -reach), reach).astype(held_as)


def heavy_noise(key, shape, deviation, limit, cuts, heavy, kind=jnp.bfloat16):
    result = deviation * jax.random.normal(key, shape, jnp.float32)
    if cuts:
        result = result * shard_levels(key, shape, cuts, -0.22, 0.18)
    return jnp.clip(strengthened(result, jax.random.fold_in(key, 3), *heavy), -limit, limit).astype(kind)


def setup_inputs(seed: int = 0) -> dict:
    streams_of = jax.random.split(jax.random.key(seed), 7)
    grads = heavy_noise(streams_of[0], (N_DP, P_SIZE), 1.0, 24.0, ((0, 256),), (0, 1, 256, 6.0), jnp.float32)
    master = draw_master(jax.random.fold_in(streams_of[6], 71), 0)
    moment1 = noise(streams_of[2], (P_SIZE,), 0.5, 4.0, ((0, 256),), jnp.float32)
    moment2 = jnp.clip(jnp.exp(math.log(2.0) - 2.9957323 * jax.random.uniform(streams_of[3], (P_SIZE,), jnp.float32) ** shard_levels(streams_of[3], (P_SIZE,), ((0, 256),), -0.2, 0.2)), 0.1, 2.0)
    tensor_rows = uneven_parts(streams_of[4], NSEG, ROWS, ROWS // 2, 2).astype(jnp.int32)
    step_count = jax.random.randint(streams_of[5], (1,), 1, 20).astype(jnp.int32)
    return dict(grads=grads, master=master, moment1=moment1, moment2=moment2, tensor_rows=tensor_rows, step_count=step_count)


def reference(grads, master, moment1, moment2, tensor_rows, step_count):
    grad = lax.optimization_barrier(jnp.sum(grads, axis=0)) / jnp.float32(N_DP)
    new_moment1 = 0.9 * moment1 + 0.1 * grad
    new_moment2 = 0.999 * moment2 + 0.001 * grad * grad
    steps = step_count[0].astype(jnp.float32)
    first = new_moment1 / (1.0 - jnp.power(jnp.float32(0.9), steps))
    second = new_moment2 / (1.0 - jnp.power(jnp.float32(0.999), steps))
    update = first / (jnp.sqrt(second) + 1e-06) + 0.1 * master
    ends = jnp.cumsum(tensor_rows).astype(jnp.int32)
    starts = ends - tensor_rows
    row_index = jnp.arange(ROWS, dtype=jnp.int32)
    onehot = ((row_index[:, None] >= starts[None, :]) & (row_index[:, None] < ends[None, :])).astype(jnp.float32)
    weight_rows = master.reshape(ROWS, D)
    update_rows = update.reshape(ROWS, D)
    row_wsq = lax.optimization_barrier(jnp.sum(weight_rows * weight_rows, axis=1))
    row_usq = lax.optimization_barrier(jnp.sum(update_rows * update_rows, axis=1))
    wsq = lax.optimization_barrier(jnp.sum(onehot * row_wsq[:, None], axis=0))
    usq = lax.optimization_barrier(jnp.sum(onehot * row_usq[:, None], axis=0))
    ratio = jnp.sqrt(wsq / (usq + 1e-06))
    row_ratio = lax.optimization_barrier(jnp.sum(onehot * ratio[None, :], axis=1))
    new_master = (weight_rows - 0.2 * row_ratio[:, None] * update_rows).reshape(P_SIZE)
    new_weights = new_master.astype(jnp.bfloat16)
    return (new_weights, new_master, new_moment1, new_moment2)
```

```python
import jax
import jax.numpy as jnp
from jax import lax
from jax.experimental import pallas as pl
from jax.experimental.pallas import tpu as pltpu
from jax.sharding import Mesh
from jax.sharding import PartitionSpec as P

AXES = ("z", "y", "x", "c")
NZ, NY, NX, NC = 8, 4, 4, 2
NSEG = 8
TILE = (5, 8, 128)
MESH_ID = pl.DeviceIdType.MESH
F32 = jnp.float32
BF16 = jnp.bfloat16


def power(base, t):
    out = jnp.float32(1.0)
    square = jnp.float32(base)
    for bit in range(5):
        out = jnp.where((t >> bit) & 1 == 1, out * square, out)
        square = square * square
    return out


def kernel(
    grads, master, moment1, moment2, rows_ref, step_ref,
    weights, out_master, out_m1, out_m2,
    gbuf, psnd, prcv, own0, own, fwd, fin, snd2, p2snd, p2rcv, col, zsnd, zrcv,
    m1v, m2v, mz, uz, ar_a, ar_b, nmv, gat,
    ld_sem, ps_sem, pr_sem, p1s_sem, p1r_sem, p2s_sem, p2r_sem,
    zs_sem, zr_sem, ms_sem, mr_sem, us_sem, ur_sem, as_sem, ar_sem, bs_sem, br_sem,
    g2s_sem, g2r_sem, g1s_sem, g1r_sem, in_sem, o_sem, ds_sem, dr_sem, ow_sem,
):
    z, y, x, c = (lax.axis_index(a) for a in AXES)
    zc = z * NC + c
    yx = y * NX + x
    other = 1 - c

    def zc_peer(i):
        t = lax.rem(zc + i, NZ * NC)
        return {"z": t // NC, "c": lax.rem(t, NC)}

    def yx_peer(i):
        t = lax.rem(yx + i, NY * NX)
        return {"y": t // NX, "x": lax.rem(t, NX)}

    barrier = pltpu.get_barrier_semaphore()

    def greet(i, carry):
        pl.semaphore_signal(barrier, inc=1, device_id=zc_peer(i), device_id_type=MESH_ID)
        pl.semaphore_signal(barrier, inc=1, device_id=yx_peer(i), device_id_type=MESH_ID)
        return carry

    lax.fori_loop(1, 16, greet, 0)

    firsts, seconds = (x, y), (y, x)
    first_axis, second_axis = ("x", "y"), ("y", "x")

    def place(p, k, j):
        t1, t2 = lax.rem(firsts[p] + k, 4), lax.rem(seconds[p] + j, 4)
        return (pl.ds(4 * p, 4), t2, t1) if p == 0 else (pl.ds(4 * p, 4), t1, t2)

    def remote(src, dst, ssem, rsem, dev):
        return pltpu.make_async_remote_copy(
            src_ref=src, dst_ref=dst, send_sem=ssem, recv_sem=rsem,
            device_id=dev, device_id_type=MESH_ID,
        )

    order = [(p, d) for d in (2, 1, 3, 0) for p in (0, 1)]
    for n, (p, d) in enumerate(order):
        for j in range(4):
            pltpu.make_async_copy(grads.at[place(p, d, j)], gbuf.at[p, d, j], ld_sem.at[p, d]).start()
        if n == 1:
            pltpu.make_async_copy(master, mz.at[z], in_sem.at[0]).start()
    pltpu.make_async_copy(moment1, m1v, in_sem.at[1]).start()
    pltpu.make_async_copy(moment2, m2v, in_sem.at[2]).start()

    pair = {
        (p, d): remote(psnd.at[p, d], prcv.at[p, d], ps_sem.at[p, d], pr_sem.at[p, d], {"c": other})
        for p, d in order
    }
    for n, (p, d) in enumerate(order):
        pltpu.make_async_copy(gbuf.at[p, d], gbuf.at[p, d], ld_sem.at[p, d]).wait()

        def cast(j, carry, p=p, d=d):
            psnd[p, d, j] = gbuf[p, d, j, :, other].astype(BF16)
            return carry

        lax.fori_loop(0, 4, cast, 0)
        if n == 0:
            pl.semaphore_wait(barrier, 30)
        pair[p, d].start()

    pltpu.make_async_copy(master, mz.at[z], in_sem.at[0]).wait()
    far_first = (4, 3, 5, 2, 6, 1, 7)

    def z_sends(src_of, dst, ssem, rsem):
        for d in far_first:
            t = lax.rem(z + d, NZ)
            remote(src_of(t), dst, ssem, rsem, {"z": t}).start()

    z_sends(lambda t: mz.at[z], mz.at[z], ms_sem, mr_sem)

    ring = {}
    for p in (0, 1):
        a, i1 = first_axis[p], firsts[p]
        right, left = {a: lax.rem(i1 + 1, 4)}, {a: lax.rem(i1 + 3, 4)}
        lo, hi = pl.ds(0, 2), pl.ds(2, 2)
        ring[p] = [
            remote(own.at[p, 1, lo], fwd.at[p, 0], p1s_sem.at[p, 0], p1r_sem.at[p, 0], right),
            remote(own.at[p, 1, hi], fwd.at[p, 1], p1s_sem.at[p, 1], p1r_sem.at[p, 1], left),
            remote(own.at[p, 0, hi], fin.at[p, 0, hi], p1s_sem.at[p, 2], p1r_sem.at[p, 2], right),
            remote(own.at[p, 2, lo], fin.at[p, 1, lo], p1s_sem.at[p, 3], p1r_sem.at[p, 3], left),
            remote(snd2.at[p, 0], fin.at[p, 0, lo], p1s_sem.at[p, 4], p1r_sem.at[p, 4], right),
            remote(snd2.at[p, 1], fin.at[p, 1, hi], p1s_sem.at[p, 5], p1r_sem.at[p, 5], left),
        ]
    for p, d in order:
        pair[p, d].wait_recv()

        def add(j, carry, p=p, d=d):
            total = gbuf[p, d, j, :, c] + prcv[p, d, j].astype(F32)
            if d == 0:
                own0[p, j] = total
            else:
                own[p, d - 1, j] = total.astype(BF16)
            return carry

        lax.fori_loop(0, 4, add, 0)
        if d == 2:
            ring[p][0].start()
            ring[p][1].start()
        elif d == 1:
            ring[p][2].start()
        elif d == 3:
            ring[p][3].start()
    for p in (0, 1):
        for way, (slot, base) in enumerate(((0, 0), (2, 2))):
            ring[p][way].wait_recv()

            def onward(j, carry, p=p, way=way, slot=slot, base=base):
                total = own[p, slot, base + j].astype(F32) + fwd[p, way, j].astype(F32)
                snd2[p, way, j] = total.astype(BF16)
                return carry

            lax.fori_loop(0, 2, onward, 0)
            ring[p][4 + way].start()

    across = {
        (p, j): remote(
            p2snd.at[p, j - 1], p2rcv.at[p, j - 1], p2s_sem.at[p, j - 1], p2r_sem.at[p, j - 1],
            {second_axis[p]: lax.rem(seconds[p] + j, 4)},
        )
        for p in (0, 1) for j in (1, 2, 3)
    }
    for p in (0, 1):
        for n in (2, 3, 4, 5):
            ring[p][n].wait_recv()
        for j in (2, 1, 3, 0):
            total = own0[p, j] + fin[p, 0, j].astype(F32) + fin[p, 1, j].astype(F32)
            if j:
                p2snd[p, j - 1] = total.astype(BF16)
                across[p, j].start()
            else:
                col[p] = total
    for p in (0, 1):
        for j in (1, 3, 2):
            across[p, j].wait_recv()
        total = col[p]
        for j in (1, 2, 3):
            total = total + p2rcv[p, j - 1].astype(F32)
        col[p] = total
        zsnd[pl.ds(4 * p, 4)] = total.astype(BF16)

    z_sends(lambda t: zsnd.at[t], zrcv.at[z], zs_sem, zr_sem)

    lane = lax.broadcasted_iota(jnp.int32, (1, 128), 1)
    starts = jnp.zeros((1, 128), jnp.int32)
    ends = jnp.zeros((1, 128), jnp.int32)
    edge = jnp.int32(0)
    for k in range(NSEG):
        starts = jnp.where(lane == k, edge, starts)
        edge = edge + rows_ref[k]
        ends = jnp.where(lane == k, edge, ends)
    my_row = (z * NY * NX + yx) * NC + c
    my_hot = jnp.where((my_row >= starts) & (my_row < ends), 1.0, 0.0).astype(F32)
    col_row = (lax.broadcasted_iota(jnp.int32, (NZ, 128), 0) * (NY * NX) + yx) * NC + c
    col_hot = jnp.where((col_row >= starts) & (col_row < ends), 1.0, 0.0).astype(F32)
    t = step_ref[0]
    scale1 = 1.0 - power(0.9, t)
    scale2 = 1.0 - power(0.999, t)
    mine = mz[z]
    my_wsq = jnp.sum(jnp.sum(jnp.sum(mine * mine, axis=0), axis=0, keepdims=True), axis=1, keepdims=True)
    pltpu.make_async_copy(moment1, m1v, in_sem.at[1]).wait()
    pltpu.make_async_copy(moment2, m2v, in_sem.at[2]).wait()

    def z_all(ref, ssem, rsem):
        return remote(ref.at[pl.ds(0, 7)], ref.at[pl.ds(0, 7)], ssem, rsem, {"z": lax.rem(z + 1, NZ)})

    z_all(zrcv, zs_sem, zr_sem).wait_recv()
    total = col[z // 4, lax.rem(z, 4)]
    for i in range(1, NZ):
        total = total + zrcv[lax.rem(z + i, NZ)].astype(F32)
    grad = total / jnp.float32(256)
    m1 = 0.9 * m1v[...] + 0.1 * grad
    m2 = 0.999 * m2v[...] + 0.001 * grad * grad
    update = (m1 / scale1) / (jnp.sqrt(m2 / scale2) + 1e-6) + 0.1 * mine
    my_usq = jnp.sum(jnp.sum(jnp.sum(update * update, axis=0), axis=0, keepdims=True), axis=1, keepdims=True)
    ar_a[zc, 0:1] = my_hot * my_usq
    ar_a[zc, 1:2] = my_hot * my_wsq
    for i in range(1, 16):
        remote(ar_a.at[zc], ar_a.at[zc], as_sem, ar_sem, zc_peer(i)).start()
    uz[z] = update
    z_sends(lambda t: uz.at[z], uz.at[z], us_sem, ur_sem)
    m1v[...] = m1
    m2v[...] = m2
    pltpu.make_async_copy(m1v, out_m1, ow_sem.at[0]).start()
    pltpu.make_async_copy(m2v, out_m2, ow_sem.at[1]).start()

    def few(ref, ssem, rsem, dev):
        return remote(ref.at[pl.ds(0, 15)], ref.at[pl.ds(0, 15)], ssem, rsem, dev)

    few(ar_a, as_sem, ar_sem, zc_peer(1)).wait_recv()
    ar_b[yx] = jnp.sum(ar_a[...], axis=0)
    for i in range(1, 16):
        remote(ar_b.at[yx], ar_b.at[yx], bs_sem, br_sem, yx_peer(i)).start()
    z_all(mz, ms_sem, mr_sem).wait_recv()
    z_all(uz, us_sem, ur_sem).wait_recv()
    few(ar_b, bs_sem, br_sem, yx_peer(1)).wait_recv()
    sums = jnp.sum(ar_b[...], axis=0)
    ratio = jnp.sqrt(sums[1:2] / (sums[0:1] + 1e-6))
    col_ratio = 0.2 * jnp.sum(col_hot * ratio, axis=1, keepdims=True)
    my_ratio = 0.2 * jnp.sum(my_hot * ratio, axis=1, keepdims=True)
    for i in range(NZ):
        factor = jnp.broadcast_to(col_ratio[i : i + 1], (8, 128))
        gat[i // 4, 0, 0, i % 4] = (mz[i] - factor * uz[i]).astype(BF16)

    def store(p, k, j):
        spot = place(p, k, j)
        pltpu.make_async_copy(gat.at[p, k, j], weights.at[(*spot, c)], o_sem).start()
        remote(gat.at[p, k, j], weights.at[(*spot, c)], ds_sem, dr_sem, {"c": other}).start()

    spread = {
        (p, d): remote(
            gat.at[p, 0, 0], gat.at[p, 0, 4 - d], g2s_sem.at[p, d - 1], g2r_sem.at[p, d - 1],
            {second_axis[p]: lax.rem(seconds[p] + d, 4)},
        )
        for p in (0, 1) for d in (1, 2, 3)
    }

    def hop(p, way, src_k, dst_k, j, n):
        a, i1 = first_axis[p], firsts[p]
        dev = {a: lax.rem(i1 + (1 if way == 0 else 3), 4)}
        return remote(
            gat.at[p, src_k, j], gat.at[p, dst_k, j], g1s_sem.at[p, way, n], g1r_sem.at[p, way, n], dev
        )

    near = {(p, w, j): hop(p, w, 0, (3, 1)[w], j, j) for p in (0, 1) for w in (0, 1) for j in range(4)}
    passed = ((0, 1), (3, 2))
    second = {
        (p, w, j): hop(p, w, (3, 1)[w], 2, j, 4 + n)
        for p in (0, 1) for w in (0, 1) for n, j in enumerate(passed[w])
    }
    for p in (0, 1):
        for d in (1, 3, 2):
            spread[p, d].start()
        for w in (0, 1):
            near[p, w, 0].start()
    nmv[...] = mine - jnp.broadcast_to(my_ratio, (8, 128)) * update
    pltpu.make_async_copy(nmv, out_master, ow_sem.at[2]).start()
    for p in (0, 1):
        store(p, 0, 0)
    for j in (1, 3, 2):
        for p in (0, 1):
            spread[p, 4 - j].wait_recv()
            for w in (0, 1):
                near[p, w, j].start()
            store(p, 0, j)
        if j == 1:
            for p in (0, 1):
                for w in (0, 1):
                    near[p, w, 0].wait_recv()
                    if 0 in passed[w]:
                        second[p, w, 0].start()
                    store(p, (3, 1)[w], 0)
    for j in (1, 3, 2):
        for p in (0, 1):
            for w in (0, 1):
                near[p, w, j].wait_recv()
                if j in passed[w]:
                    second[p, w, j].start()
                store(p, (3, 1)[w], j)
    for n in (0, 1):
        for p in (0, 1):
            for w in (0, 1):
                j = passed[w][n]
                second[p, w, j].wait_recv()
                store(p, 2, j)

    for p, d in order:
        pair[p, d].wait_send()
    for p in (0, 1):
        for copy in ring[p]:
            copy.wait_send()
    for group in (across, spread, near, second):
        for copy in group.values():
            copy.wait_send()
    z_all(mz, ms_sem, mr_sem).wait_send()
    z_all(zrcv, zs_sem, zr_sem).wait_send()
    z_all(uz, us_sem, ur_sem).wait_send()
    few(ar_a, as_sem, ar_sem, zc_peer(1)).wait_send()
    few(ar_b, bs_sem, br_sem, yx_peer(1)).wait_send()
    pltpu.make_async_copy(m1v, out_m1, ow_sem.at[0]).wait()
    pltpu.make_async_copy(m2v, out_m2, ow_sem.at[1]).wait()
    pltpu.make_async_copy(nmv, out_master, ow_sem.at[2]).wait()
    half = weights.at[:, :, :, c]
    pltpu.make_async_copy(half, half, o_sem).wait()
    both = remote(half, half, ds_sem, dr_sem, {"c": other})
    both.wait_send()
    both.wait_recv()


def body(grads, master, moment1, moment2, tensor_rows, step_count):
    any_space = pl.BlockSpec(memory_space=pl.ANY)
    smem = pl.BlockSpec(memory_space=pltpu.SMEM)
    full = (NZ, NY, NX, NC, *TILE)
    block = jax.ShapeDtypeStruct(TILE, F32)
    dma = pltpu.SemaphoreType.DMA
    vm = pltpu.VMEM
    scratch = [
        vm((2, 4, 4, 4, 2, *TILE), F32),
        vm((2, 4, 4, 4, *TILE), BF16),
        vm((2, 4, 4, 4, *TILE), BF16),
        vm((2, 4, 4, *TILE), F32),
        vm((2, 3, 4, 4, *TILE), BF16),
        vm((2, 2, 2, 4, *TILE), BF16),
        vm((2, 2, 4, 4, *TILE), BF16),
        vm((2, 2, 2, 4, *TILE), BF16),
        vm((2, 3, 4, *TILE), BF16),
        vm((2, 3, 4, *TILE), BF16),
        vm((2, 4, *TILE), F32),
        vm((NZ, *TILE), BF16),
        vm((NZ, *TILE), BF16),
        vm(TILE, F32),
        vm(TILE, F32),
        vm((NZ, *TILE), F32),
        vm((NZ, *TILE), F32),
        vm((16, 2, 128), F32),
        vm((16, 2, 128), F32),
        vm(TILE, F32),
        vm((2, 4, 4, 4, *TILE), BF16),
        dma((2, 4)), dma((2, 4)), dma((2, 4)), dma((2, 6)), dma((2, 6)), dma((2, 3)), dma((2, 3)),
        dma, dma, dma, dma, dma, dma, dma, dma, dma, dma,
        dma((2, 3)), dma((2, 3)), dma((2, 2, 6)), dma((2, 2, 6)), dma((3,)), dma, dma, dma, dma((3,)),
    ]
    weights, new_master, new_m1, new_m2 = pl.pallas_call(
        kernel,
        out_shape=(jax.ShapeDtypeStruct(full, BF16), block, block, block),
        in_specs=[any_space] * 4 + [smem] * 2,
        out_specs=(any_space,) * 4,
        scratch_shapes=scratch,
        compiler_params=pltpu.CompilerParams(
            collective_id=0, has_side_effects=True, vmem_limit_bytes=40 * 1024 * 1024
        ),
    )(
        grads.reshape(full), master.reshape(TILE), moment1.reshape(TILE), moment2.reshape(TILE),
        tensor_rows, step_count,
    )
    return (weights.reshape(-1), new_master.reshape(-1), new_m1.reshape(-1), new_m2.reshape(-1))


def solution(mesh):
    torus = Mesh(mesh.devices.reshape(NZ, NY, NX, NC), AXES)
    placed = (P(AXES, None), P(AXES), P(AXES), P(AXES), P(), P())
    return jax.shard_map(
        body, mesh=torus, in_specs=placed, out_specs=(P(), P(AXES), P(AXES), P(AXES)), check_vma=False
    )
```

```python
import jax
import jax.numpy as jnp
from jax import lax
from jax.experimental import pallas as pl
from jax.experimental.pallas import tpu as pltpu
from jax.sharding import Mesh
from jax.sharding import PartitionSpec as P

AXES = ("z", "y", "x", "c")
NZ, NY, NX, NC = 8, 4, 4, 2
NSEG = 8
TILE = (5, 8, 128)
MESH_ID = pl.DeviceIdType.MESH
F32 = jnp.float32
BF16 = jnp.bfloat16


def power(base, t):
    out = jnp.float32(1.0)
    square = jnp.float32(base)
    for bit in range(5):
        out = jnp.where((t >> bit) & 1 == 1, out * square, out)
        square = square * square
    return out


def kernel(
    grads, master, moment1, moment2, rows_hbm, step_ref,
    weights, out_master, out_m1, out_m2,
    gbuf, psnd, prcv, own0, own, fwd, fin, snd2, p2snd, p2rcv, col, zsnd, zrcv,
    rows_ref, m1v, m2v, mz, uz, ar_a, ar_b,
    ld_sem, ps_sem, pr_sem, p1s_sem, p1r_sem, p2s_sem, p2r_sem,
    zs_sem, zr_sem, ms_sem, mr_sem, us_sem, ur_sem, as_sem, ar_sem, bs_sem, br_sem,
    g2s_sem, g2r_sem, g1s_sem, g1r_sem, in_sem, ds_sem, dr_sem,
):
    z, y, x, c = (lax.axis_index(a) for a in AXES)
    zc = z * NC + c
    yx = y * NX + x
    other = 1 - c

    def zc_peer(i):
        t = lax.rem(zc + i, NZ * NC)
        return {"z": t // NC, "c": lax.rem(t, NC)}

    def yx_peer(i):
        t = lax.rem(yx + i, NY * NX)
        return {"y": t // NX, "x": lax.rem(t, NX)}

    barrier = pltpu.get_barrier_semaphore()

    def greet(i, carry):
        pl.semaphore_signal(barrier, inc=1, device_id=zc_peer(i), device_id_type=MESH_ID)
        pl.semaphore_signal(barrier, inc=1, device_id=yx_peer(i), device_id_type=MESH_ID)
        return carry

    lax.fori_loop(1, 16, greet, 0)

    firsts, seconds = (x, y), (y, x)
    first_axis, second_axis = ("x", "y"), ("y", "x")

    def place(p, k, j):
        t1, t2 = lax.rem(firsts[p] + k, 4), lax.rem(seconds[p] + j, 4)
        return (pl.ds(4 * p, 4), t2, t1) if p == 0 else (pl.ds(4 * p, 4), t1, t2)

    def remote(src, dst, ssem, rsem, dev):
        return pltpu.make_async_remote_copy(
            src_ref=src, dst_ref=dst, send_sem=ssem, recv_sem=rsem,
            device_id=dev, device_id_type=MESH_ID,
        )

    order = [(p, d) for d in (2, 1, 3, 0) for p in (0, 1)]
    for n, (p, d) in enumerate(order):
        for j in range(4):
            pltpu.make_async_copy(grads.at[place(p, d, j)], gbuf.at[p, d, j], ld_sem.at[p, d]).start()
        if n == 1:
            pltpu.make_async_copy(master, mz.at[z], in_sem.at[0]).start()
    pltpu.make_async_copy(moment1, m1v, in_sem.at[1]).start()
    pltpu.make_async_copy(moment2, m2v, in_sem.at[2]).start()
    pltpu.make_async_copy(rows_hbm, rows_ref, in_sem.at[3]).start()

    pair = {
        (p, d): remote(psnd.at[p, d], prcv.at[p, d], ps_sem.at[p, d], pr_sem.at[p, d], {"c": other})
        for p, d in order
    }
    for n, (p, d) in enumerate(order):
        pltpu.make_async_copy(gbuf.at[p, d], gbuf.at[p, d], ld_sem.at[p, d]).wait()

        def cast(j, carry, p=p, d=d):
            psnd[p, d, j] = gbuf[p, d, j, :, other].astype(BF16)
            return carry

        lax.fori_loop(0, 4, cast, 0)
        if n == 0:
            pl.semaphore_wait(barrier, 30)
        pair[p, d].start()

    pltpu.make_async_copy(master, mz.at[z], in_sem.at[0]).wait()
    far_first = (4, 3, 5, 2, 6, 1, 7)

    def z_sends(src_of, dst, ssem, rsem):
        for d in far_first:
            t = lax.rem(z + d, NZ)
            remote(src_of(t), dst, ssem, rsem, {"z": t}).start()

    z_sends(lambda t: mz.at[z], mz.at[z], ms_sem, mr_sem)

    ring = {}
    for p in (0, 1):
        a, i1 = first_axis[p], firsts[p]
        right, left = {a: lax.rem(i1 + 1, 4)}, {a: lax.rem(i1 + 3, 4)}
        lo, hi = pl.ds(0, 2), pl.ds(2, 2)
        ring[p] = [
            remote(own.at[p, 1, lo], fwd.at[p, 0], p1s_sem.at[p, 0], p1r_sem.at[p, 0], right),
            remote(own.at[p, 1, hi], fwd.at[p, 1], p1s_sem.at[p, 1], p1r_sem.at[p, 1], left),
            remote(own.at[p, 0, hi], fin.at[p, 0, hi], p1s_sem.at[p, 2], p1r_sem.at[p, 2], right),
            remote(own.at[p, 2, lo], fin.at[p, 1, lo], p1s_sem.at[p, 3], p1r_sem.at[p, 3], left),
            remote(snd2.at[p, 0], fin.at[p, 0, lo], p1s_sem.at[p, 4], p1r_sem.at[p, 4], right),
            remote(snd2.at[p, 1], fin.at[p, 1, hi], p1s_sem.at[p, 5], p1r_sem.at[p, 5], left),
        ]
    for p, d in order:
        pair[p, d].wait_recv()

        def add(j, carry, p=p, d=d):
            total = gbuf[p, d, j, :, c] + prcv[p, d, j].astype(F32)
            if d == 0:
                own0[p, j] = total
            else:
                own[p, d - 1, j] = total.astype(BF16)
            return carry

        lax.fori_loop(0, 4, add, 0)
        if d == 2:
            ring[p][0].start()
            ring[p][1].start()
        elif d == 1:
            ring[p][2].start()
        elif d == 3:
            ring[p][3].start()
    for p in (0, 1):
        for way, (slot, base) in enumerate(((0, 0), (2, 2))):
            ring[p][way].wait_recv()

            def onward(j, carry, p=p, way=way, slot=slot, base=base):
                total = own[p, slot, base + j].astype(F32) + fwd[p, way, j].astype(F32)
                snd2[p, way, j] = total.astype(BF16)
                return carry

            lax.fori_loop(0, 2, onward, 0)
            ring[p][4 + way].start()

    across = {
        (p, j): remote(
            p2snd.at[p, j - 1], p2rcv.at[p, j - 1], p2s_sem.at[p, j - 1], p2r_sem.at[p, j - 1],
            {second_axis[p]: lax.rem(seconds[p] + j, 4)},
        )
        for p in (0, 1) for j in (1, 2, 3)
    }
    for p in (0, 1):
        for n in (2, 3, 4, 5):
            ring[p][n].wait_recv()
        for j in (2, 1, 3, 0):
            total = own0[p, j] + fin[p, 0, j].astype(F32) + fin[p, 1, j].astype(F32)
            if j:
                p2snd[p, j - 1] = total.astype(BF16)
                across[p, j].start()
            else:
                col[p] = total
    for p in (0, 1):
        for j in (1, 3, 2):
            across[p, j].wait_recv()
        total = col[p]
        for j in (1, 2, 3):
            total = total + p2rcv[p, j - 1].astype(F32)
        col[p] = total
        zsnd[pl.ds(4 * p, 4)] = total.astype(BF16)

    z_sends(lambda t: zsnd.at[t], zrcv.at[z], zs_sem, zr_sem)

    pltpu.make_async_copy(rows_hbm, rows_ref, in_sem.at[3]).wait()
    lane = lax.broadcasted_iota(jnp.int32, (1, 128), 1)
    starts = jnp.zeros((1, 128), jnp.int32)
    ends = jnp.zeros((1, 128), jnp.int32)
    edge = jnp.int32(0)
    for k in range(NSEG):
        starts = jnp.where(lane == k, edge, starts)
        edge = edge + rows_ref[k]
        ends = jnp.where(lane == k, edge, ends)
    my_row = (z * NY * NX + yx) * NC + c
    my_hot = jnp.where((my_row >= starts) & (my_row < ends), 1.0, 0.0).astype(F32)
    col_row = (lax.broadcasted_iota(jnp.int32, (NZ, 128), 0) * (NY * NX) + yx) * NC + c
    col_hot = jnp.where((col_row >= starts) & (col_row < ends), 1.0, 0.0).astype(F32)
    t = step_ref[0]
    scale1 = 1.0 - power(0.9, t)
    scale2 = 1.0 - power(0.999, t)
    mine = mz[z]
    my_wsq = jnp.sum(jnp.sum(jnp.sum(mine * mine, axis=0), axis=0, keepdims=True), axis=1, keepdims=True)
    pltpu.make_async_copy(moment1, m1v, in_sem.at[1]).wait()
    pltpu.make_async_copy(moment2, m2v, in_sem.at[2]).wait()

    def z_all(ref, ssem, rsem):
        return remote(ref.at[pl.ds(0, 7)], ref.at[pl.ds(0, 7)], ssem, rsem, {"z": lax.rem(z + 1, NZ)})

    z_all(zrcv, zs_sem, zr_sem).wait_recv()
    total = col[z // 4, lax.rem(z, 4)]
    for i in range(1, NZ):
        total = total + zrcv[lax.rem(z + i, NZ)].astype(F32)
    grad = total / jnp.float32(256)
    m1 = 0.9 * m1v[...] + 0.1 * grad
    m2 = 0.999 * m2v[...] + 0.001 * grad * grad
    update = (m1 / scale1) / (jnp.sqrt(m2 / scale2) + 1e-6) + 0.1 * mine
    my_usq = jnp.sum(jnp.sum(jnp.sum(update * update, axis=0), axis=0, keepdims=True), axis=1, keepdims=True)
    ar_a[zc, 0:1] = my_hot * my_usq
    ar_a[zc, 1:2] = my_hot * my_wsq
    for i in range(1, 16):
        remote(ar_a.at[zc], ar_a.at[zc], as_sem, ar_sem, zc_peer(i)).start()
    uz[z] = update
    z_sends(lambda t: uz.at[z], uz.at[z], us_sem, ur_sem)
    out_m1[...] = m1
    out_m2[...] = m2

    def few(ref, ssem, rsem, dev):
        return remote(ref.at[pl.ds(0, 15)], ref.at[pl.ds(0, 15)], ssem, rsem, dev)

    few(ar_a, as_sem, ar_sem, zc_peer(1)).wait_recv()
    ar_b[yx] = jnp.sum(ar_a[...], axis=0)
    for i in range(1, 16):
        remote(ar_b.at[yx], ar_b.at[yx], bs_sem, br_sem, yx_peer(i)).start()
    z_all(mz, ms_sem, mr_sem).wait_recv()
    z_all(uz, us_sem, ur_sem).wait_recv()
    few(ar_b, bs_sem, br_sem, yx_peer(1)).wait_recv()
    sums = jnp.sum(ar_b[...], axis=0)
    ratio = jnp.sqrt(sums[1:2] / (sums[0:1] + 1e-6))
    col_ratio = 0.2 * jnp.sum(col_hot * ratio, axis=1, keepdims=True)
    my_ratio = 0.2 * jnp.sum(my_hot * ratio, axis=1, keepdims=True)
    for i in range(NZ):
        factor = jnp.broadcast_to(col_ratio[i : i + 1], (8, 128))
        weights[i, y, x, c] = (mz[i] - factor * uz[i]).astype(BF16)

    def spot(p, k, j):
        return weights.at[(*place(p, k, j), c)]

    def store(p, k, j):
        remote(spot(p, k, j), spot(p, k, j), ds_sem, dr_sem, {"c": other}).start()

    def spread_copy(p, j, d):
        return remote(
            spot(p, 0, j), spot(p, 0, j), g2s_sem.at[p, d - 1], g2r_sem.at[p, d - 1],
            {second_axis[p]: lax.rem(seconds[p] + d, 4)},
        )

    def hop(p, way, k, j, n):
        dev = {first_axis[p]: lax.rem(firsts[p] + (1 if way == 0 else 3), 4)}
        return remote(spot(p, k, j), spot(p, k, j), g1s_sem.at[p, way, n], g1r_sem.at[p, way, n], dev)

    passed = ((0, 1), (3, 2))
    pd = [(p, d) for p in (0, 1) for d in (1, 2, 3)]
    pwj = [(p, w, j) for p in (0, 1) for w in (0, 1) for j in range(4)]
    pwn = [(p, w, n) for p in (0, 1) for w in (0, 1) for n in (0, 1)]
    spread_sent = {(p, d): spread_copy(p, 0, d) for p, d in pd}
    spread_here = {(p, 4 - d): spread_copy(p, 4 - d, d) for p, d in pd}
    near_sent = {(p, w, j): hop(p, w, 0, j, j) for p, w, j in pwj}
    near_here = {(p, w, j): hop(p, w, (3, 1)[w], j, j) for p, w, j in pwj}
    second_sent = {(p, w, passed[w][n]): hop(p, w, (3, 1)[w], passed[w][n], 4 + n) for p, w, n in pwn}
    second_here = {(p, w, passed[w][n]): hop(p, w, 2, passed[w][n], 4 + n) for p, w, n in pwn}
    for p in (0, 1):
        for d in (1, 3, 2):
            spread_sent[p, d].start()
        for w in (0, 1):
            near_sent[p, w, 0].start()
    out_master[...] = mine - jnp.broadcast_to(my_ratio, (8, 128)) * update
    for p in (0, 1):
        store(p, 0, 0)
    for j in (1, 3, 2):
        for p in (0, 1):
            spread_here[p, j].wait_recv()
            for w in (0, 1):
                near_sent[p, w, j].start()
            store(p, 0, j)
        if j == 1:
            for p in (0, 1):
                for w in (0, 1):
                    near_here[p, w, 0].wait_recv()
                    if 0 in passed[w]:
                        second_sent[p, w, 0].start()
                    store(p, (3, 1)[w], 0)
    for j in (1, 3, 2):
        for p in (0, 1):
            for w in (0, 1):
                near_here[p, w, j].wait_recv()
                if j in passed[w]:
                    second_sent[p, w, j].start()
                store(p, (3, 1)[w], j)
    for n in (0, 1):
        for p in (0, 1):
            for w in (0, 1):
                j = passed[w][n]
                second_here[p, w, j].wait_recv()
                store(p, 2, j)

    for p, d in order:
        pair[p, d].wait_send()
    for p in (0, 1):
        for copy in ring[p]:
            copy.wait_send()
    for group in (across, spread_sent, near_sent, second_sent):
        for copy in group.values():
            copy.wait_send()
    z_all(mz, ms_sem, mr_sem).wait_send()
    z_all(zrcv, zs_sem, zr_sem).wait_send()
    z_all(uz, us_sem, ur_sem).wait_send()
    few(ar_a, as_sem, ar_sem, zc_peer(1)).wait_send()
    few(ar_b, bs_sem, br_sem, yx_peer(1)).wait_send()
    half = weights.at[:, :, :, c]
    both = remote(half, half, ds_sem, dr_sem, {"c": other})
    both.wait_send()
    both.wait_recv()


def write_out(*refs):
    copies = [pltpu.make_async_copy(refs[i], refs[4 + i], refs[8].at[i]) for i in range(4)]
    for copy in copies:
        copy.start()
    for copy in copies:
        copy.wait()


def body(grads, master, moment1, moment2, tensor_rows, step_count):
    hbm = pl.BlockSpec(memory_space=pltpu.HBM)
    vmem = pl.BlockSpec(memory_space=pltpu.VMEM)
    full = (NZ, NY, NX, NC, *TILE)
    block = jax.ShapeDtypeStruct(TILE, F32)
    dma = pltpu.SemaphoreType.DMA
    vm = pltpu.VMEM
    scratch = [
        vm((2, 4, 4, 4, 2, *TILE), F32),
        vm((2, 4, 4, 4, *TILE), BF16),
        vm((2, 4, 4, 4, *TILE), BF16),
        vm((2, 4, 4, *TILE), F32),
        vm((2, 3, 4, 4, *TILE), BF16),
        vm((2, 2, 2, 4, *TILE), BF16),
        vm((2, 2, 4, 4, *TILE), BF16),
        vm((2, 2, 2, 4, *TILE), BF16),
        vm((2, 3, 4, *TILE), BF16),
        vm((2, 3, 4, *TILE), BF16),
        vm((2, 4, *TILE), F32),
        vm((NZ, *TILE), BF16),
        vm((NZ, *TILE), BF16),
        pltpu.SMEM((NSEG,), jnp.int32),
        vm(TILE, F32),
        vm(TILE, F32),
        vm((NZ, *TILE), F32),
        vm((NZ, *TILE), F32),
        vm((16, 2, 128), F32),
        vm((16, 2, 128), F32),
        dma((2, 4)), dma((2, 4)), dma((2, 4)), dma((2, 6)), dma((2, 6)), dma((2, 3)), dma((2, 3)),
        dma, dma, dma, dma, dma, dma, dma, dma, dma, dma,
        dma((2, 3)), dma((2, 3)), dma((2, 2, 6)), dma((2, 2, 6)), dma((4,)), dma, dma,
    ]
    shapes = (jax.ShapeDtypeStruct(full, BF16), block, block, block)
    def keep(a):
        return pltpu.with_memory_space_constraint(a, pltpu.HBM)

    made = pl.pallas_call(
        kernel,
        out_shape=shapes,
        in_specs=[hbm] * 5 + [pl.BlockSpec(memory_space=pltpu.SMEM)],
        out_specs=(vmem,) * 4,
        scratch_shapes=scratch,
        compiler_params=pltpu.CompilerParams(
            collective_id=0, has_side_effects=True, vmem_limit_bytes=40 * 1024 * 1024
        ),
    )(
        keep(grads.reshape(full)), keep(master.reshape(TILE)), keep(moment1.reshape(TILE)),
        keep(moment2.reshape(TILE)), keep(tensor_rows), step_count,
    )
    weights, new_master, new_m1, new_m2 = pl.pallas_call(
        write_out,
        out_shape=shapes,
        in_specs=[vmem] * 4,
        out_specs=(hbm,) * 4,
        scratch_shapes=[dma((4,))],
        compiler_params=pltpu.CompilerParams(vmem_limit_bytes=8 * 1024 * 1024),
    )(*made)
    return (weights.reshape(-1), new_master.reshape(-1), new_m1.reshape(-1), new_m2.reshape(-1))


def solution(mesh):
    torus = Mesh(mesh.devices.reshape(NZ, NY, NX, NC), AXES)
    placed = (P(AXES, None), P(AXES), P(AXES), P(AXES), P(), P())
    return jax.shard_map(
        body, mesh=torus, in_specs=placed, out_specs=(P(), P(AXES), P(AXES), P(AXES)), check_vma=False
    )
```
